32 devices in a mesh: bank: 4 (over z), zero: 8 (over y, x, core).
Axes of the slice: x: 2, y: 2, z: 4, core: 2. Of those that a mesh axis runs over, the one named last changes fastest.
Arguments:
- master_gate: float32 [64, 2048, 1024], P('bank', 'zero'), may hold values from -0.1875 to 0.1875
- second_gate: bfloat16 [64, 2048, 1024], P('bank', 'zero'), may hold values from -0.0625 to 0.0625
- master_up: float32 [64, 2048, 1024], P('bank', 'zero'), may hold values from -0.1875 to 0.1875
- second_up: bfloat16 [64, 2048, 1024], P('bank', 'zero'), may hold values from -0.0625 to 0.0625
- master_down: float32 [64, 1024, 2048], P('bank', None, 'zero'), may hold values from -0.25 to 0.25
- second_down: bfloat16 [64, 1024, 2048], P('bank', None, 'zero'), may hold values from -0.09375 to 0.09375
- router_weight: float32 [2048, 64], P('zero', 'bank'), may hold values from -0.125 to 0.125
- router_gain: float32 [2048], P('zero'), may hold values from 0.25 to 1.75
Outputs:
- final_gate: bfloat16 [64, 2048, 1024], P('bank', None, 'zero')
- final_up: bfloat16 [64, 2048, 1024], P('bank', None, 'zero')
- final_down: bfloat16 [64, 1024, 2048], P('bank', 'zero')
- scale_gate: float32 [64, 1024], P('bank', 'zero')
- scale_up: float32 [64, 1024], P('bank', 'zero')
- scale_down: float32 [64, 1024], P('bank', 'zero')
- serve_router: bfloat16 [2048, 64], replicated
The draws below stay inside these ranges and needn't reach their ends.
All inputs are finite; a program needn't handle non-finite values. Where the reference program divides by a largest or mean magnitude, that divisor is 1e-20 or more.
Results may differ from the reference program's by a relative error of at most 0.001.
Values may be sent and summed in bfloat16 or wider, within the bound.
A program may use at most 192 MiB of HBM per device.

```python
import jax
import jax.numpy as jnp

EXPERTS = 64
D_MODEL = 2048
D_EXPERT = 1024


def strengthened(array, own_key, source, target, blocks, factor):
    def block_of(dim):
        return (jnp.arange(array.shape[dim]) // (array.shape[dim] // blocks)).reshape((-1,) + (1,) * (array.ndim - 1 - dim))

    one_side = jax.random.permutation(own_key, blocks)[block_of(target)]
    other_side = (block_of(target) + blocks // 2) % blocks
    return jnp.where((block_of(source) == one_side) | (block_of(source) == other_side), factor * array, array)


def levels(rng, extent, cuts, smallest, largest):
    def one(dim, parts):
        heights = jax.random.uniform(jax.random.fold_in(jax.random.fold_in(rng, 6), dim), (parts,), jnp.float32, smallest / len(cuts), largest / len(cuts))
        return jnp.repeat(jnp.exp(heights), extent[dim] // parts).reshape((-1,) + (1,) * (len(extent) - dim - 1))

    factor_of = one(*cuts[0])
    for cut in cuts[1:]:
        factor_of = factor_of * one(*cut)
    return factor_of


def gaussian(key, extent, scale, limit, shards=(), dtype=jnp.bfloat16):
    values = scale * jax.random.normal(key, extent, jnp.float32)
    if shards:
        values = values * levels(key, extent, shards, -0.22, 0.18)
    return jnp.clip(values, -limit, limit).astype(dtype)


def bell_draw_with(stream_key, dims, width, reach, cuts, heavy, dtype=jnp.bfloat16):
    drawn = width * jax.random.normal(stream_key, dims, jnp.float32)
    if cuts:
        drawn = drawn * levels(stream_key, dims, cuts, -0.22, 0.18)
    return jnp.clip(strengthened(drawn, jax.random.fold_in(stream_key, 3), *heavy), -reach, reach).astype(dtype)


def setup_inputs(seed: int = 0) -> dict:
    keys = jax.random.split(jax.random.key(seed), 9)
    return {
        "master_gate": bell_draw_with(keys[0], (EXPERTS, D_MODEL, D_EXPERT), D_MODEL ** -0.5, 0.1875, ((0, 4), (1, 8)), (1, 2, 8, 2.0), jnp.float32),
        "second_gate": gaussian(keys[1], (EXPERTS, D_MODEL, D_EXPERT), (D_MODEL * 4) ** -0.5, 0.0625, ((0, 4), (1, 8))),
        "master_up": bell_draw_with(keys[2], (EXPERTS, D_MODEL, D_EXPERT), D_MODEL ** -0.5, 0.1875, ((0, 4), (1, 8)), (1, 2, 8, 2.0), jnp.float32),
        "second_up": gaussian(keys[3], (EXPERTS, D_MODEL, D_EXPERT), (D_MODEL * 4) ** -0.5, 0.0625, ((0, 4), (1, 8))),
        "master_down": bell_draw_with(keys[4], (EXPERTS, D_EXPERT, D_MODEL), D_EXPERT ** -0.5, 0.25, ((0, 4), (2, 8)), (2, 1, 8, 2.0), jnp.float32),
        "second_down": gaussian(keys[5], (EXPERTS, D_EXPERT, D_MODEL), (D_EXPERT * 4) ** -0.5, 0.09375, ((0, 4), (2, 8))),
        "router_weight": gaussian(keys[6], (D_MODEL, EXPERTS), D_MODEL ** -0.5, 0.125, ((0, 8), (1, 4)), jnp.float32),
        "router_gain": jnp.clip(1.0 + 0.15 * jax.random.normal(keys[7], (D_MODEL,), jnp.float32), 0.25, 1.75),
    }


def reference(master_gate, second_gate, master_up, second_up, master_down, second_down, router_weight, router_gain):
    merged_gate = master_gate + second_gate.astype(jnp.float32)
    merged_up = master_up + second_up.astype(jnp.float32)
    merged_down = master_down + second_down.astype(jnp.float32)
    scale_gate = jnp.sum(jnp.abs(merged_gate), axis=1) / D_MODEL
    final_gate = (merged_gate / jnp.expand_dims(scale_gate, 1)).astype(jnp.bfloat16)
    scale_up = jnp.sum(jnp.abs(merged_up), axis=1) / D_MODEL
    final_up = (merged_up / jnp.expand_dims(scale_up, 1)).astype(jnp.bfloat16)
    scale_down = jnp.sum(jnp.abs(merged_down), axis=2) / D_MODEL
    final_down = (merged_down / jnp.expand_dims(scale_down, 2)).astype(jnp.bfloat16)
    serve_router = (router_weight * router_gain[:, None]).astype(jnp.bfloat16)
    return final_gate, final_up, final_down, scale_gate, scale_up, scale_down, serve_router
```

```python
import jax
import jax.numpy as jnp
from jax import lax
from jax.experimental import pallas as pl
from jax.experimental.pallas import tpu as pltpu
from jax.sharding import PartitionSpec as P

f32, bf16 = jnp.float32, jnp.bfloat16


def cost(read_write, flops):
    return pl.CostEstimate(flops=flops, bytes_accessed=read_write, transcendentals=0)


def to_all(part, axes, count):
    same = jnp.broadcast_to(part[None], (count,) + part.shape)
    return lax.all_to_all(same, axes, split_axis=0, concat_axis=0, tiled=True)


def narrow_columns(master, second, inverse, zero):
    experts, rows, width = master.shape
    piece = width // zero
    step = 2 if experts % 2 == 0 else 1

    def body(master_ref, second_ref, inverse_ref, out_ref):
        for k in range(zero):
            cut = slice(k * piece, (k + 1) * piece)
            merged = master_ref[:, :, cut] + second_ref[:, :, cut].astype(f32)
            out_ref[k] = (merged * inverse_ref[:, :, cut]).astype(bf16)

    block = pl.BlockSpec((step, rows, width), lambda i: (i, 0, 0))
    return pl.pallas_call(
        body,
        grid=(experts // step,),
        in_specs=[block, block, pl.BlockSpec((step, 1, width), lambda i: (i, 0, 0))],
        out_specs=pl.BlockSpec((zero, step, rows, piece), lambda i: (0, i, 0, 0)),
        out_shape=jax.ShapeDtypeStruct((zero, experts, rows, piece), bf16),
        cost_estimate=cost(8 * master.size, 2 * master.size),
    )(master, second, inverse)


def join(pieces, axis):
    zero, experts, rows, columns = pieces.shape
    step = 2 if experts % 2 == 0 else 1
    shape = (zero * rows, columns) if axis == 1 else (rows, zero * columns)

    def body(in_ref, out_ref):
        for k in range(zero):
            if axis == 1:
                out_ref[:, k * rows : (k + 1) * rows, :] = in_ref[k]
            else:
                out_ref[:, :, k * columns : (k + 1) * columns] = in_ref[k]

    return pl.pallas_call(
        body,
        grid=(experts // step,),
        in_specs=[pl.BlockSpec((zero, step, rows, columns), lambda i: (0, i, 0, 0))],
        out_specs=pl.BlockSpec((step,) + shape, lambda i: (i, 0, 0)),
        out_shape=jax.ShapeDtypeStruct((experts,) + shape, pieces.dtype),
        cost_estimate=cost(4 * pieces.size, 0),
    )(pieces)


def exchange(pieces):
    return lax.all_to_all(pieces, "zero", split_axis=0, concat_axis=0, tiled=True)


def mine(scale, zero):
    width = scale.shape[1] // zero
    return lax.dynamic_slice_in_dim(scale, lax.axis_index("zero") * width, width, axis=1)


def aligned_device(sizes, mg, sg, mu, su, md, sd, router_weight, router_gain):
    bank, zero = sizes
    experts, rows, width = mg.shape
    model = rows * zero

    part_router = (router_weight * router_gain[:, None]).astype(bf16)
    router = to_all(part_router.reshape(-1, 128), ("bank", "zero"), bank * zero)

    part_up = jnp.sum(jnp.abs(mu + su.astype(f32)), axis=1)
    part_up, router = lax.optimization_barrier((part_up, router))
    all_up = to_all(part_up, "zero", zero)
    all_gate = to_all(jnp.sum(jnp.abs(mg + sg.astype(f32)), axis=1), "zero", zero)
    merged_down = md + sd.astype(f32)
    part_down = jnp.sum(jnp.abs(merged_down), axis=2)
    all_gate, all_up, part_down = lax.optimization_barrier((all_gate, all_up, part_down))
    all_down = to_all(part_down, "zero", zero)

    scale_gate = jnp.sum(all_gate, axis=0) / model
    narrow_gate = narrow_columns(mg, sg, (1.0 / scale_gate)[:, None, :], zero)
    narrow_gate, all_up, all_down = lax.optimization_barrier((narrow_gate, all_up, all_down))
    got_gate = exchange(narrow_gate)

    scale_up = jnp.sum(all_up, axis=0) / model
    narrow_up = narrow_columns(mu, su, (1.0 / scale_up)[:, None, :], zero)
    got_up = exchange(narrow_up)

    scale_down = jnp.sum(all_down, axis=0) / model
    narrow_down = (merged_down * (1.0 / scale_down)[:, :, None]).astype(bf16)
    split_down = narrow_down.reshape(experts, zero, width // zero, rows).transpose(1, 0, 2, 3)
    got_down = exchange(split_down)

    serve_router = (
        router.reshape(bank, zero, *part_router.shape).transpose(1, 2, 0, 3).reshape(model, -1)
    )
    return (
        join(got_gate, 1),
        join(got_up, 1),
        join(got_down, 2),
        mine(scale_gate, zero),
        mine(scale_up, zero),
        mine(scale_down, zero),
        serve_router,
    )


def general_device(sizes, mg, sg, mu, su, md, sd, router_weight, router_gain):
    zero = sizes[1]
    model = mg.shape[1] * zero
    merged = (mg + sg.astype(f32), mu + su.astype(f32), md + sd.astype(f32))
    totals = lax.psum(
        tuple(jnp.sum(jnp.abs(m), axis=a) for m, a in zip(merged, (1, 1, 2))), "zero"
    )
    scales = tuple(t / model for t in totals)
    finals = tuple(
        lax.all_to_all(
            (m / jnp.expand_dims(s, a)).astype(bf16),
            "zero", split_axis=3 - a, concat_axis=a, tiled=True,
        )
        for m, s, a in zip(merged, scales, (1, 1, 2))
    )
    part_router = (router_weight * router_gain[:, None]).astype(bf16)
    row_router = lax.all_gather(part_router, "zero", axis=0, tiled=True)
    serve_router = lax.all_gather(row_router, "bank", axis=1, tiled=True)
    return finals + tuple(mine(s, zero) for s in scales) + (serve_router,)


def solution(mesh):
    sizes = (mesh.shape["bank"], mesh.shape["zero"])

    def on_device(*args):
        _, rows, width = args[0].shape
        piece = width // sizes[1]
        tiles = piece % 128 == 0 and rows % 128 == 0 and args[6].size % 128 == 0
        return (aligned_device if tiles else general_device)(sizes, *args)

    return jax.shard_map(
        on_device,
        mesh=mesh,
        in_specs=(
            P("bank", "zero", None),
            P("bank", "zero", None),
            P("bank", "zero", None),
            P("bank", "zero", None),
            P("bank", None, "zero"),
            P("bank", None, "zero"),
            P("zero", "bank"),
            P("zero"),
        ),
        out_specs=(
            P("bank", None, "zero"),
            P("bank", None, "zero"),
            P("bank", "zero", None),
            P("bank", "zero"),
            P("bank", "zero"),
            P("bank", "zero"),
            P(),
        ),
        check_vma=False,
    )
```
